32 devices in a mesh: seq: 32 (over z, y, x, core), head: 1.
Axes of the slice: x: 2, y: 2, z: 4, core: 2. Of those that a mesh axis runs over, the one named last changes fastest.
Arguments:
- queries: bfloat16 [8192, 4096], P('seq', 'head'), may hold values from -8 to 8
- keys: bfloat16 [8192, 1024], P('seq', 'head'), may hold values from -8 to 8
- values: bfloat16 [8192, 1024], P('seq', 'head'), may hold values from -8 to 8
- gate_logit: float32 [32], P('head'), may hold values from -3 to 3
- out_weight: bfloat16 [4096, 4096], P('head'), may hold values from -0.09375 to 0.09375
Outputs:
- layer_out: bfloat16 [8192, 4096], P('seq', 'head')
The draws below stay inside these ranges and needn't reach their ends.
All inputs are finite; a program needn't handle non-finite values.
Results may differ from the reference program's by a relative error of at most 0.0095.
Values may be sent and summed in bfloat16 or wider, within the bound.
A program may use at most 320 MiB of HBM per device.

```python
import math
import jax
import jax.numpy as jnp
from jax import lax

D = 4096
Q_HEADS = 32
KV_HEADS = 8
HDIM = 128
WINDOW = 4096
SEG = 1024
TOK_DEV = 256
TOKENS = 8192


def draw_queries(key, part):
    base_key = jax.random.fold_in(key, 11)
    base_draw = jnp.clip(0.6 * jax.random.normal(base_key, (TOKENS, Q_HEADS, HDIM), jnp.float32), -8.0, 8.0)
    return base_draw.reshape(TOKENS, Q_HEADS * HDIM).astype(jnp.bfloat16)


def draw_keys(key, part):
    scale_key = jax.random.fold_in(key, 21)
    token_key = jax.random.fold_in(key, 22)
    base_key = jax.random.fold_in(key, 23)
    block_scale = jnp.exp(jax.random.uniform(scale_key, (TOKENS // TOK_DEV, KV_HEADS), jnp.float32, math.log(0.3), math.log(3.0)))
    block_scale = jnp.repeat(block_scale, TOK_DEV, axis=0)
    token_scale = jnp.exp(jax.random.uniform(token_key, (TOKENS, KV_HEADS), jnp.float32, math.log(0.6), math.log(1.6)))
    row_scale = (block_scale * token_scale)[:, :, None]
    base_draw = jax.random.normal(base_key, (TOKENS, KV_HEADS, HDIM), jnp.float32)
    base_draw = jnp.clip(base_draw * row_scale, -8.0, 8.0)
    return base_draw.reshape(TOKENS, KV_HEADS * HDIM).astype(jnp.bfloat16)


def draw_values(key, part):
    offset_key = jax.random.fold_in(key, 31)
    base_key = jax.random.fold_in(key, 32)
    offsets = jax.random.uniform(offset_key, (TOKENS // TOK_DEV, KV_HEADS * HDIM), jnp.float32, -1.0, 1.0)
    offsets = jnp.repeat(offsets, TOK_DEV, axis=0)
    base_draw = jax.random.normal(base_key, (TOKENS, KV_HEADS * HDIM), jnp.float32)
    return jnp.clip(base_draw + offsets, -8.0, 8.0).astype(jnp.bfloat16)


def centred(own_key, extent, width, limit, held_as=jnp.bfloat16):
    return jnp.clip(width * jax.random.normal(own_key, extent, jnp.float32), -limit, limit).astype(held_as)


def setup_inputs(seed: int = 0) -> dict:
    seeds = jax.random.split(jax.random.key(seed), 6)
    return {
        "queries": draw_queries(jax.random.fold_in(seeds[5], 71), 0),
        "keys": draw_keys(jax.random.fold_in(seeds[5], 71), 0),
        "values": draw_values(jax.random.fold_in(seeds[5], 71), 0),
        "gate_logit": jnp.clip(jax.random.uniform(seeds[3], (Q_HEADS,), jnp.float32, -3.0, 3.0), -3.0, 3.0),
        "out_weight": centred(seeds[4], (Q_HEADS * HDIM, D), (Q_HEADS * HDIM) ** -0.5, 0.09375),
    }


def feature(source):
    return jax.nn.elu(source.astype(jnp.float32)) + 1.0

def reference(queries, keys, values, gate_logit, out_weight):
    group_size = Q_HEADS // KV_HEADS
    score_scale = 1.0 / math.sqrt(HDIM)
    query_four = queries.reshape(TOKENS, KV_HEADS, group_size, HDIM)
    key_three = keys.reshape(TOKENS, KV_HEADS, HDIM)
    value_three = values.reshape(TOKENS, KV_HEADS, HDIM)
    padding = jnp.zeros((WINDOW, KV_HEADS, HDIM), jnp.bfloat16)
    key_padded = jnp.concatenate([padding, key_three], 0)
    value_padded = jnp.concatenate([padding, value_three], 0)

    def attend_block(block):
        first = (block * TOK_DEV).astype(jnp.int32)
        query_rows = lax.dynamic_slice_in_dim(query_four, first, TOK_DEV, 0).astype(jnp.float32)
        key_rows = lax.dynamic_slice_in_dim(key_padded, first, WINDOW + TOK_DEV, 0).astype(jnp.float32)
        value_rows = lax.dynamic_slice_in_dim(value_padded, first, WINDOW + TOK_DEV, 0).astype(jnp.float32)
        query_pos = first + jnp.arange(TOK_DEV, dtype=jnp.int32)
        key_pos = first - WINDOW + jnp.arange(WINDOW + TOK_DEV, dtype=jnp.int32)
        distance = query_pos[:, None] - key_pos[None, :]
        allowed = (distance >= 0) & (distance < WINDOW) & (key_pos[None, :] >= 0)
        scores = jnp.einsum('tgrd,sgd->tgrs', query_rows, key_rows) * score_scale
        scores = jnp.where(allowed[:, None, None, :], scores, jnp.float32(-1e+30))
        peak = lax.optimization_barrier(jnp.max(scores, axis=-1, keepdims=True))
        weights = jnp.exp(scores - peak)
        sum_total = lax.optimization_barrier(jnp.sum(weights, axis=-1))
        low = weights.astype(jnp.bfloat16).astype(jnp.float32)
        weighted = jnp.einsum('tgrs,sgd->tgrd', low, value_rows)
        return weighted / sum_total[..., None]
    local_out = lax.map(attend_block, jnp.arange(TOKENS // TOK_DEV, dtype=jnp.int32))
    local_out = local_out.reshape(TOKENS, KV_HEADS, group_size, HDIM)
    seg_count = TOKENS // SEG
    key_feature = feature(key_three).astype(jnp.bfloat16).astype(jnp.float32).reshape(seg_count, SEG, KV_HEADS, HDIM)
    value_seg = value_three.astype(jnp.float32).reshape(seg_count, SEG, KV_HEADS, HDIM)
    delta_memory = jnp.einsum('nsgd,nsge->ngde', key_feature, value_seg, precision=lax.Precision.HIGHEST)
    delta_norm = lax.optimization_barrier(jnp.sum(key_feature, axis=1))
    memory = jnp.concatenate([jnp.zeros((1, KV_HEADS, HDIM, HDIM), jnp.float32), jnp.cumsum(delta_memory, 0)[:-1]], 0)
    key_total = jnp.concatenate([jnp.zeros((1, KV_HEADS, HDIM), jnp.float32), jnp.cumsum(delta_norm, 0)[:-1]], 0)
    query_feature = feature(query_four).astype(jnp.bfloat16).astype(jnp.float32).reshape(seg_count, SEG, KV_HEADS, group_size, HDIM)
    recalled = jnp.einsum('nsgrd,ngde->nsgre', query_feature, memory, precision=lax.Precision.HIGHEST)
    denominator = 1.0 + jnp.einsum('nsgrd,ngd->nsgr', query_feature, key_total, precision=lax.Precision.HIGHEST)
    retrieved = (recalled / denominator[..., None]).reshape(TOKENS, KV_HEADS, group_size, HDIM)
    gate_share = jax.nn.sigmoid(gate_logit.astype(jnp.float32)).reshape(KV_HEADS, group_size)[None, :, :, None]
    mixed = (gate_share * retrieved + (1.0 - gate_share) * local_out).astype(jnp.bfloat16)
    mixed = mixed.reshape(TOKENS, Q_HEADS * HDIM)
    return jnp.dot(mixed, out_weight, preferred_element_type=jnp.float32).astype(jnp.bfloat16)
```

```python
import functools
import math

import jax
import jax.numpy as jnp
from jax import lax
from jax.experimental import pallas as pl
from jax.experimental.pallas import tpu as pltpu
from jax.sharding import PartitionSpec as P

HDIM = 128
WINDOW = 4096
SEG = 1024
LOG2E = 1.4426950408889634
EXP_SCALE = LOG2E / math.sqrt(HDIM)
TILE = 512
PAD = 16
ZB, ZC, BX, BY, BYF, AX, AY, AXF = range(8)
KV = (0, 1)


def feature(source):
    wide = source.astype(jnp.float32)
    low = jnp.exp(jnp.minimum(wide, 0.0))
    return jnp.where(wide > 0.0, wide + 1.0, low)


def kernel(
    size, group_size, gate_ref, q_hbm, k_hbm, v_hbm, w_hbm, out_ref,
    qbuf, kbuf, vbuf, m_ref, acc_ref, mix, wbuf, psend, precv, pown,
    wsend, wrecv, dsum, dpre,
    local_sem, xsend, xrecv, send_sem, recv_sem, dsend, drecv, psem, prsem,
):
    rows = q_hbm.shape[0]
    heads = kbuf.shape[0]
    width = heads * HDIM
    qwidth = width * group_size
    own_q = heads * group_size
    blocks = 2 * group_size
    tiles = w_hbm.shape[1] // TILE
    me = lax.axis_index("seq")
    plane = me // 8
    p = me % 8
    core = p % 2
    xbit = (p // 2) % 2
    ybit = p // 4
    j = p // 2
    j_x = j + 1 - 2 * xbit
    j_y = j + 2 - 4 * ybit
    dev_core = me + 1 - 2 * core
    dev_x = me + 2 - 4 * xbit
    dev_y = me + 4 - 8 * ybit
    bufs = (kbuf, vbuf)
    has_up = me + 8 < size
    has_down = plane >= 1
    two_down = plane >= 2

    def remote(src, dst, ssem, rsem, dev):
        return pltpu.make_async_remote_copy(
            src_ref=src, dst_ref=dst, send_sem=ssem, recv_sem=rsem,
            device_id={"seq": dev}, device_id_type=pl.DeviceIdType.MESH,
        )

    plan = {
        ZB: (j, 4 + j, me + 8, has_up, has_down),
        ZC: (4 + j, 8, me + 8, has_up & has_down, two_down),
        BX: (4 + j, 4 + j, dev_x, has_down, has_down),
        BY: (4 + j, 4 + j, dev_y, has_down, has_down),
        BYF: (4 + j_x, 4 + j_x, dev_y, has_down, has_down),
        AX: (j + xbit * (8 - j), j, dev_x, (xbit == 0) | two_down, (xbit == 1) | two_down),
        AY: (j + ybit * (8 - j), j, dev_y, (ybit == 0) | two_down, (ybit == 1) | two_down),
        AXF: (j_y, j_y, dev_x, (ybit == 1) | two_down, (ybit == 1) | two_down),
    }

    def copy_of(kind, h, kv):
        src, dst, dev, _, _ = plan[kind]
        return remote(
            bufs[kv].at[h, src], bufs[kv].at[h, dst],
            send_sem.at[kind, h, kv], recv_sem.at[kind, h, kv], dev,
        )

    def start(kind, h, also=None):
        ok = plan[kind][3] if also is None else plan[kind][3] & also

        @pl.when(ok)
        def _():
            for kv in KV:
                copy_of(kind, h, kv).start()

    def arrive(kind, h):
        @pl.when(plan[kind][4])
        def _():
            for kv in KV:
                copy_of(kind, h, kv).wait_recv()

    def event_0(h):
        start(ZB, h)
        start(AX, h, xbit == 0)
        start(AY, h, ybit == 0)

    def event_1(h):
        arrive(ZB, h)
        start(BX, h)
        start(BY, h)
        start(ZC, h)

    def event_2(h):
        arrive(ZC, h)
        start(AX, h, xbit == 1)
        start(AY, h, ybit == 1)

    def event_3(h):
        arrive(BX, h)
        start(BYF, h)

    def event_4(h):
        arrive(AY, h)
        start(AXF, h)

    def when_head(h, event):
        @pl.when(h < heads)
        def _():
            event(h)

    def delta_copy(i):
        dev = (dev_x, dev_y, me + 8)[i]
        return remote(wsend.at[i], wrecv.at[i], dsend.at[i], drecv.at[i], dev)

    def delta_send(i, value):
        wsend[i] = value.astype(jnp.bfloat16)
        delta_copy(i).start()

    def delta_arrive(i):
        delta_copy(i).wait_recv()
        return wrecv[i].astype(jnp.float32)

    def attend(h, slot, mask=None):
        qk_dims = (((1,), (1,)), ((), ()))

        def span(half):
            if mask == "own" and half == 0:
                return 0, rows
            if mask == "old" and half == 1:
                return rows, rows
            return 0, 2 * rows

        def block(i):
            return slice(i * rows, (i + 1) * rows)

        def scores(i):
            first, count = span(i % 2)
            cols = pl.ds(pl.multiple_of((h * group_size + i // 2) * HDIM, HDIM), HDIM)
            q = qbuf[(i % 2) * rows:(i % 2 + 1) * rows, cols]
            s = lax.dot_general(
                q, kbuf[h, slot, first:first + count, :], qk_dims,
                preferred_element_type=jnp.float32,
            )
            if mask is None:
                return s
            qpos = lax.broadcasted_iota(jnp.int32, (rows, rows), 0)
            kpos = lax.broadcasted_iota(jnp.int32, (rows, rows), 1)
            allowed = (qpos >= kpos) if mask == "own" else (kpos > qpos)
            low = jnp.float32(-1e30)
            if count == rows:
                return jnp.where(allowed, s, low)
            if mask == "own":
                return jnp.concatenate([s[:, :rows], jnp.where(allowed, s[:, rows:], low)], axis=1)
            return jnp.concatenate([jnp.where(allowed, s[:, :rows], low), s[:, rows:]], axis=1)

        def soften(i, s):
            top = jnp.max(s, axis=1, keepdims=True)
            shape = (rows, HDIM)
            if mask == "own":
                new, alpha = jnp.broadcast_to(top, shape), None
            else:
                old = m_ref[block(i), :]
                new = jnp.maximum(old, top)
                alpha = jnp.exp2((old - new) * EXP_SCALE)
            m_ref[block(i), :] = new
            shift = jnp.concatenate([new] * (s.shape[1] // HDIM), axis=1)
            return jnp.exp2((s - shift) * EXP_SCALE).astype(jnp.bfloat16), alpha

        def gather(i, w, alpha):
            first, count = span(i % 2)
            v = vbuf[h, slot, first:first + count, :]
            wide = jnp.concatenate([v, jnp.ones((count, HDIM), jnp.bfloat16)], axis=1)
            pv = jnp.dot(w, wide, preferred_element_type=jnp.float32)
            if alpha is None:
                acc_ref[block(i), :] = pv
            else:
                acc_ref[block(i), :] = (
                    acc_ref[block(i), :] * jnp.concatenate([alpha, alpha], axis=1) + pv
                )

        waiting, ready = {}, {}
        for t in range(blocks + 2):
            if t < blocks:
                waiting[t] = scores(t)
            if 0 <= t - 1 < blocks:
                ready[t - 1] = soften(t - 1, waiting.pop(t - 1))
            if 0 <= t - 2 < blocks:
                gather(t - 2, *ready.pop(t - 2))

    def finish(h):
        cols = pl.ds(pl.multiple_of(h * HDIM, HDIM), HDIM)
        mem = dpre[0:HDIM, cols]
        high = mem.astype(jnp.bfloat16)
        low = (mem - high.astype(jnp.float32)).astype(jnp.bfloat16)
        norm = dpre[HDIM:HDIM + 1, cols]

        def one(r, carry):
            n = h * group_size + r
            qcols = pl.ds(pl.multiple_of(n * HDIM, HDIM), HDIM)
            arows = pl.ds(pl.multiple_of(r * (2 * rows), 2 * rows), 2 * rows)
            qf = feature(qbuf[:, qcols]).astype(jnp.bfloat16)
            recalled = jnp.dot(qf, high, preferred_element_type=jnp.float32) + jnp.dot(
                qf, low, preferred_element_type=jnp.float32
            )
            denominator = 1.0 + jnp.sum(qf.astype(jnp.float32) * norm, axis=1, keepdims=True)
            local_out = acc_ref[arows, 0:HDIM] / acc_ref[arows, HDIM:]
            share = gate_ref[core * own_q + n]
            mixed = share * (recalled / denominator) + (1.0 - share) * local_out
            mix[:, qcols] = mixed.astype(jnp.bfloat16)
            return carry

        lax.fori_loop(0, group_size, one, 0)

    mine = pl.ds(pl.multiple_of(core * rows, rows), rows)
    hbms = (k_hbm, v_hbm)

    def head_cols(owner, h):
        return pl.ds(pl.multiple_of((owner * heads + h) * HDIM, HDIM), HDIM)

    def half_cols(owner):
        return pl.ds(pl.multiple_of(owner * qwidth, qwidth), qwidth)

    local, swaps = [], []
    for h in range(heads):
        for kv in KV:
            i = 2 * h + kv
            place = bufs[kv].at[h, j, mine, :]
            local.append(pltpu.make_async_copy(
                hbms[kv].at[:, head_cols(core, h)], place, local_sem.at[i]))
            swaps.append(remote(
                hbms[kv].at[:, head_cols(1 - core, h)], place, xsend.at[i], xrecv.at[i], dev_core))
    local.append(pltpu.make_async_copy(
        q_hbm.at[:, half_cols(core)], qbuf.at[mine, :], local_sem.at[2 * heads]))
    swaps.append(remote(
        q_hbm.at[:, half_cols(1 - core)], qbuf.at[mine, :],
        xsend.at[2 * heads], xrecv.at[2 * heads], dev_core))
    weights = pltpu.make_async_copy(
        w_hbm.at[pl.ds(pl.multiple_of(core * qwidth, qwidth), qwidth), :], wbuf,
        local_sem.at[2 * heads + 1])

    for c in local:
        c.start()
    barrier = pltpu.get_barrier_semaphore()
    for dev in (dev_core, dev_x, dev_y):
        pl.semaphore_signal(
            barrier, inc=1, device_id={"seq": dev}, device_id_type=pl.DeviceIdType.MESH
        )

    @pl.when(has_up)
    def _():
        pl.semaphore_signal(
            barrier, inc=1, device_id={"seq": me + 8}, device_id_type=pl.DeviceIdType.MESH
        )

    @pl.when(has_down)
    def _():
        pl.semaphore_signal(
            barrier, inc=1, device_id={"seq": me - 8}, device_id_type=pl.DeviceIdType.MESH
        )

    steps = max(size // 8 - 1, 1)
    neighbours_up = 1 - plane // steps if size > 8 else 0
    neighbours_down = (plane + steps - 1) // steps if size > 8 else 0
    pl.semaphore_wait(barrier, 3 + neighbours_up + jnp.minimum(neighbours_down, 1))

    for c in swaps:
        c.start()
    weights.start()
    for c in local:
        c.wait()
    for c in swaps:
        c.wait_recv()

    event_0(0)
    for h in range(heads):
        cols = slice(h * HDIM, (h + 1) * HDIM)
        kf = feature(kbuf[h, j]).astype(jnp.bfloat16)
        dsum[0:HDIM, cols] = lax.dot_general(
            kf, vbuf[h, j], (((0,), (0,)), ((), ())), preferred_element_type=jnp.float32
        )
        norm = jnp.sum(kf.astype(jnp.float32), axis=0, keepdims=True)
        dsum[HDIM:, cols] = jnp.broadcast_to(norm, (PAD, HDIM))
    delta_send(0, dsum[...])
    event_1(0)
    event_0(1)
    dsum[...] += delta_arrive(0)
    delta_send(1, dsum[...])
    event_2(0)
    event_3(0)
    other = delta_arrive(1)
    dpre[...] = other * ybit.astype(jnp.float32)
    dsum[...] += other

    @pl.when(has_up & (plane == 0))
    def _():
        delta_send(2, dsum[...])

    event_4(0)

    def chain():
        @pl.when(has_down)
        def _():
            before = delta_arrive(2)
            dpre[...] += before

            @pl.when(has_up)
            def _():
                delta_send(2, before + dsum[...])

    def xor(a_bit, b_bit):
        return a_bit + b_bit - 2 * a_bit * b_bit

    def one_head(h, carry):
        attend(h, j, "own")
        when_head(h + 1, event_1)

        def step(s, c):
            late = s // 4
            t = s - 3 * late
            slot = 4 * (1 - late) + xor(xbit, t % 2) + 2 * xor(ybit, t // 2)

            @pl.when(s == 1)
            def _():
                when_head(h + 2, event_0)

            @pl.when(s == 2)
            def _():
                arrive(BY, h)

            @pl.when(s == 3)
            def _():
                when_head(h + 1, event_2)
                when_head(h + 1, event_3)
                arrive(BYF, h)

                @pl.when(h == 0)
                def _():
                    chain()

            @pl.when(s == 4)
            def _():
                arrive(AX, h)

            @pl.when(s == 5)
            def _():
                when_head(h + 1, event_4)

            @pl.when(s == 6)
            def _():
                arrive(AXF, h)

            bit = jnp.where(s == 4, xbit, ybit)
            valid = ((s < 4) & has_down) | ((s >= 4) & ((bit == 1) | two_down))

            @pl.when(valid)
            def _():
                attend(h, slot)

            return c

        lax.fori_loop(0, 7, step, 0)

        @pl.when(two_down)
        def _():
            attend(h, 8, "old")

        finish(h)
        return carry

    lax.fori_loop(0, heads, one_head, 0)

    weights.wait()
    theirs = pl.ds(pl.multiple_of((1 - core) * rows, rows), rows)

    def partial_copy(i):
        return remote(psend.at[i], precv.at[i], psem.at[i], prsem.at[i], dev_core)

    def project(i, carry):
        cols = pl.ds(pl.multiple_of(i * TILE, TILE), TILE)
        psend[i] = jnp.dot(mix[theirs, :], wbuf[:, cols], preferred_element_type=jnp.float32)
        partial_copy(i).start()
        return carry

    def project_own(i, carry):
        cols = pl.ds(pl.multiple_of(i * TILE, TILE), TILE)
        pown[...] = jnp.dot(mix[mine, :], wbuf[:, cols], preferred_element_type=jnp.float32)
        partial_copy(i).wait_recv()
        out_ref[:, cols] = (pown[...] + precv[i]).astype(jnp.bfloat16)
        return carry

    lax.fori_loop(0, tiles, project, 0)
    lax.fori_loop(0, tiles, project_own, 0)

    def sent(i, carry):
        partial_copy(i).wait_send()
        return carry

    lax.fori_loop(0, tiles, sent, 0)
    for c in swaps:
        c.wait_send()
    for i in (0, 1):
        delta_copy(i).wait_send()

    @pl.when(has_up)
    def _():
        delta_copy(2).wait_send()

    def all_sent(h, carry):
        for kind in plan:
            @pl.when(plan[kind][3])
            def _(kind=kind):
                for kv in KV:
                    copy_of(kind, h, kv).wait_send()
        return carry

    lax.fori_loop(0, heads, all_sent, 0)


def per_device(size, queries, keys, values, gate_logit, out_weight):
    rows = queries.shape[0]
    heads = gate_logit.shape[0]
    groups = keys.shape[1] // HDIM
    group_size = heads // groups
    assert WINDOW == 16 * rows and SEG == 4 * rows and size % 8 == 0 and groups % 2 == 0
    mine = groups // 2
    columns = out_weight.shape[1]
    qwidth = mine * group_size * HDIM
    tiles = columns // TILE
    f32, bf16 = jnp.float32, jnp.bfloat16
    vmem, anywhere = pl.BlockSpec(memory_space=pltpu.VMEM), pl.BlockSpec(memory_space=pl.ANY)
    dma = pltpu.SemaphoreType.DMA
    partial_value = pl.pallas_call(
        functools.partial(kernel, size, group_size),
        out_shape=jax.ShapeDtypeStruct((rows, columns), bf16),
        in_specs=[pl.BlockSpec(memory_space=pltpu.SMEM)] + [anywhere] * 4,
        out_specs=vmem,
        scratch_shapes=[
            pltpu.VMEM((2 * rows, qwidth), bf16),
            pltpu.VMEM((mine, 9, 2 * rows, HDIM), bf16),
            pltpu.VMEM((mine, 9, 2 * rows, HDIM), bf16),
            pltpu.VMEM((2 * rows * group_size, HDIM), f32),
            pltpu.VMEM((2 * rows * group_size, 2 * HDIM), f32),
            pltpu.VMEM((2 * rows, qwidth), bf16),
            pltpu.VMEM((qwidth, columns), bf16),
            pltpu.VMEM((tiles, rows, TILE), f32),
            pltpu.VMEM((tiles, rows, TILE), f32),
            pltpu.VMEM((rows, TILE), f32),
            pltpu.VMEM((3, HDIM + PAD, mine * HDIM), bf16),
            pltpu.VMEM((3, HDIM + PAD, mine * HDIM), bf16),
            pltpu.VMEM((HDIM + PAD, mine * HDIM), f32),
            pltpu.VMEM((HDIM + PAD, mine * HDIM), f32),
            dma((2 * mine + 2,)),
            dma((2 * mine + 1,)),
            dma((2 * mine + 1,)),
            dma((8, mine, 2)),
            dma((8, mine, 2)),
            dma((3,)),
            dma((3,)),
            dma((tiles,)),
            dma((tiles,)),
        ],
        compiler_params=pltpu.CompilerParams(
            collective_id=0, has_side_effects=True, vmem_limit_bytes=60 * 1024 * 1024
        ),
    )(jax.nn.sigmoid(gate_logit), queries, keys, values, out_weight)
    return lax.psum_scatter(partial_value, "head", scatter_dimension=1, tiled=True)


def solution(mesh):
    in_specs = (P("seq", "head"), P("seq", "head"), P("seq", "head"), P("head"), P("head", None))
    out_specs = P("seq", "head")
    return jax.shard_map(
        functools.partial(per_device, mesh.shape["seq"]),
        mesh=mesh, in_specs=in_specs, out_specs=out_specs, check_vma=False,
    )
```

```python
import functools
import math

import jax
import jax.numpy as jnp
from jax import lax
from jax.experimental import pallas as pl
from jax.experimental.pallas import tpu as pltpu
from jax.sharding import PartitionSpec as P

HDIM = 128
WINDOW = 4096
SEG = 1024
LOG2E = 1.4426950408889634
EXP_SCALE = LOG2E / math.sqrt(HDIM)
TILE = 1024
PAD = 16
ZB, ZC, BX, BY, BYF, AX, AY, AXF = range(8)
KV = (0, 1)


def feature(source):
    wide = source.astype(jnp.float32)
    low = jnp.exp(jnp.minimum(wide, 0.0))
    return jnp.where(wide > 0.0, wide + 1.0, low)


def kernel(
    size, group_size, gate_ref, q_hbm, k_hbm, v_hbm, w_hbm, out_ref,
    qbuf, kbuf, vbuf, m_ref, acc_ref, mix, msend, wbuf, pown,
    wsend, wrecv, dsum, dpre,
    local_sem, xsend, xrecv, send_sem, recv_sem, dsend, drecv, psem, prsem, wsem,
):
    rows = q_hbm.shape[0]
    heads = kbuf.shape[0]
    width = heads * HDIM
    gwidth = group_size * HDIM
    qwidth = width * group_size
    own_q = heads * group_size
    blocks = 2 * group_size
    tiles = w_hbm.shape[1] // TILE
    me = lax.axis_index("seq")
    plane = me // 8
    p = me % 8
    core = p % 2
    xbit = (p // 2) % 2
    ybit = p // 4
    j = p // 2
    j_x = j + 1 - 2 * xbit
    j_y = j + 2 - 4 * ybit
    dev_core = me + 1 - 2 * core
    dev_x = me + 2 - 4 * xbit
    dev_y = me + 4 - 8 * ybit
    bufs = (kbuf, vbuf)
    has_up = me + 8 < size
    has_down = plane >= 1
    two_down = plane >= 2

    def remote(src, dst, ssem, rsem, dev):
        return pltpu.make_async_remote_copy(
            src_ref=src, dst_ref=dst, send_sem=ssem, recv_sem=rsem,
            device_id={"seq": dev}, device_id_type=pl.DeviceIdType.MESH,
        )

    plan = {
        ZB: (j, 4 + j, me + 8, has_up, has_down),
        ZC: (4 + j, 8, me + 8, has_up & has_down, two_down),
        BX: (4 + j, 4 + j, dev_x, has_down, has_down),
        BY: (4 + j, 4 + j, dev_y, has_down, has_down),
        BYF: (4 + j_x, 4 + j_x, dev_y, has_down, has_down),
        AX: (j + xbit * (8 - j), j, dev_x, (xbit == 0) | two_down, (xbit == 1) | two_down),
        AY: (j + ybit * (8 - j), j, dev_y, (ybit == 0) | two_down, (ybit == 1) | two_down),
        AXF: (j_y, j_y, dev_x, (ybit == 1) | two_down, (ybit == 1) | two_down),
    }

    def copy_of(kind, h, kv):
        src, dst, dev, _, _ = plan[kind]
        return remote(
            bufs[kv].at[h, src], bufs[kv].at[h, dst],
            send_sem.at[kind, h, kv], recv_sem.at[kind, h, kv], dev,
        )

    def start(kind, h, also=None, kvs=KV):
        ok = plan[kind][3] if also is None else plan[kind][3] & also

        @pl.when(ok)
        def _():
            for kv in kvs:
                copy_of(kind, h, kv).start()

    def arrive(kind, h, kvs=KV):
        @pl.when(plan[kind][4])
        def _():
            for kv in kvs:
                copy_of(kind, h, kv).wait_recv()

    def relay(kind, onward, h):
        for kv in KV:
            arrive(kind, h, (kv,))
            start(onward, h, None, (kv,))

    def open_head(h):
        arrive(ZC, h)
        for kind in (BX, AY, AX, BY):
            start(kind, h)

    def when_head(h, event):
        @pl.when(h < heads)
        def _():
            event(h)

    def delta_copy(i):
        dev = (dev_x, dev_y, me + 8)[i]
        return remote(wsend.at[i], wrecv.at[i], dsend.at[i], drecv.at[i], dev)

    def delta_send(i, value):
        wsend[i] = value.astype(jnp.bfloat16)
        delta_copy(i).start()

    def delta_arrive(i):
        delta_copy(i).wait_recv()
        return wrecv[i].astype(jnp.float32)

    def attend(h, slots, mask=None):
        qk_dims = (((1,), (1,)), ((), ()))

        def span(half):
            if mask == "own" and half == 0:
                return 0, rows
            if mask == "old" and half == 1:
                return rows, rows
            return 0, 2 * rows

        def block(i):
            return slice(i * rows, (i + 1) * rows)

        def scores(i):
            first, count = span(i % 2)
            cols = pl.ds(pl.multiple_of((h * group_size + i // 2) * HDIM, HDIM), HDIM)
            q = qbuf[(i % 2) * rows:(i % 2 + 1) * rows, cols]
            parts = [
                lax.dot_general(
                    q, kbuf[h, slot, first:first + count, :], qk_dims,
                    preferred_element_type=jnp.float32,
                )
                for slot in slots
            ]
            if mask is None:
                return jnp.concatenate(parts, axis=1) if len(parts) > 1 else parts[0]
            s, = parts
            qpos = lax.broadcasted_iota(jnp.int32, (rows, rows), 0)
            kpos = lax.broadcasted_iota(jnp.int32, (rows, rows), 1)
            allowed = (qpos >= kpos) if mask == "own" else (kpos > qpos)
            low = jnp.float32(-1e30)
            if count == rows:
                return jnp.where(allowed, s, low)
            if mask == "own":
                return jnp.concatenate([s[:, :rows], jnp.where(allowed, s[:, rows:], low)], axis=1)
            return jnp.concatenate([jnp.where(allowed, s[:, :rows], low), s[:, rows:]], axis=1)

        def soften(i, s):
            top = jnp.max(s, axis=1, keepdims=True)
            shape = (rows, HDIM)
            if mask == "own":
                new, alpha = jnp.broadcast_to(top, shape), None
            else:
                old = m_ref[block(i), :]
                new = jnp.maximum(old, top)
                alpha = jnp.exp2((old - new) * EXP_SCALE)
            m_ref[block(i), :] = new
            shift = jnp.concatenate([new] * (s.shape[1] // HDIM), axis=1)
            return jnp.exp2((s - shift) * EXP_SCALE).astype(jnp.bfloat16), alpha

        def gather(i, w, alpha):
            first, count = span(i % 2)
            pv = None
            for k, slot in enumerate(slots):
                v = vbuf[h, slot, first:first + count, :]
                wide = jnp.concatenate([v, jnp.ones((count, HDIM), jnp.bfloat16)], axis=1)
                one = jnp.dot(
                    w[:, k * count:(k + 1) * count], wide, preferred_element_type=jnp.float32
                )
                pv = one if pv is None else pv + one
            if alpha is None:
                acc_ref[h % 2, block(i), :] = pv
            else:
                acc_ref[h % 2, block(i), :] = (
                    acc_ref[h % 2, block(i), :] * jnp.concatenate([alpha, alpha], axis=1) + pv
                )

        waiting, ready = {}, {}
        for t in range(blocks + 2):
            if t < blocks:
                waiting[t] = scores(t)
            if 0 <= t - 1 < blocks:
                ready[t - 1] = soften(t - 1, waiting.pop(t - 1))
            if 0 <= t - 2 < blocks:
                gather(t - 2, *ready.pop(t - 2))

    def finish(h):
        cols = pl.ds(pl.multiple_of(h * HDIM, HDIM), HDIM)
        mem = dpre[0:HDIM, cols]
        high = mem.astype(jnp.bfloat16)
        low = (mem - high.astype(jnp.float32)).astype(jnp.bfloat16)
        norm = dpre[HDIM:HDIM + 1, cols]

        def part(place, target):
            def one(r, carry):
                n = h * group_size + r
                qcols = pl.ds(pl.multiple_of(n * HDIM, HDIM), HDIM)
                arows = pl.ds(pl.multiple_of((2 * r + place) * rows, rows), rows)
                qrows = pl.ds(pl.multiple_of(place * rows, rows), rows)
                qf = feature(qbuf[qrows, qcols]).astype(jnp.bfloat16)
                recalled = jnp.dot(qf, high, preferred_element_type=jnp.float32) + jnp.dot(
                    qf, low, preferred_element_type=jnp.float32
                )
                denominator = 1.0 + jnp.sum(qf.astype(jnp.float32) * norm, axis=1, keepdims=True)
                local_out = acc_ref[h % 2, arows, 0:HDIM] / acc_ref[h % 2, arows, HDIM:]
                share = jax.nn.sigmoid(jnp.full((1, HDIM), gate_ref[core * own_q + n], jnp.float32))
                mixed = share * (recalled / denominator) + (1.0 - share) * local_out
                target[:, pl.ds(pl.multiple_of(r * HDIM, HDIM), HDIM)] = mixed.astype(jnp.bfloat16)
                return carry

            lax.fori_loop(0, group_size, one, 0)

        part(1 - core, msend.at[h])
        mix_copy(h).start()
        part(core, mix.at[h, 0])

    def mix_copy(h):
        return remote(msend.at[h], mix.at[h, 1], psem.at[h], prsem.at[h], dev_core)

    def product(h, side, cols):
        return jnp.dot(mix[h, side], wbuf[h % 2, side, :, cols], preferred_element_type=jnp.float32)

    def weights(h):
        for side in (0, 1):
            owner = core + side * (1 - 2 * core)
            wrows = pl.ds(pl.multiple_of((owner * heads + h) * gwidth, gwidth), gwidth)
            yield pltpu.make_async_copy(w_hbm.at[wrows, :], wbuf.at[h % 2, side], wsem.at[h, side])

    def fetch(h):
        for c in weights(h):
            c.start()

    def fetched(h):
        for c in weights(h):
            c.wait()

    def tile_cols(i):
        return pl.ds(pl.multiple_of(i * TILE, TILE), TILE)

    def project(h):
        mix_copy(h).wait_recv()
        fetched(h)

        def one(i, carry):
            cols = tile_cols(i)
            pown[:, cols] += product(h, 0, cols) + product(h, 1, cols)
            return carry

        lax.fori_loop(0, tiles, one, 0)
        when_head(h + 2, fetch)

    def project_last(h):
        fetched(h)

        def one(i, carry):
            cols = tile_cols(i)
            pown[:, cols] += product(h, 0, cols)
            return carry

        lax.fori_loop(0, tiles, one, 0)
        mix_copy(h).wait_recv()

        def two(i, carry):
            cols = tile_cols(i)
            out_ref[:, cols] = (pown[:, cols] + product(h, 1, cols)).astype(jnp.bfloat16)
            return carry

        lax.fori_loop(0, tiles, two, 0)

    mine = pl.ds(pl.multiple_of(core * rows, rows), rows)
    hbms = (k_hbm, v_hbm)

    def head_cols(owner, h):
        return pl.ds(pl.multiple_of((owner * heads + h) * HDIM, HDIM), HDIM)

    def half_cols(owner):
        return pl.ds(pl.multiple_of(owner * qwidth, qwidth), qwidth)

    local, swaps = [], []
    for h in range(heads):
        for kv in KV:
            i = 2 * h + kv
            place = bufs[kv].at[h, j, mine, :]
            local.append(pltpu.make_async_copy(
                hbms[kv].at[:, head_cols(core, h)], place, local_sem.at[i]))
            swaps.append(remote(
                hbms[kv].at[:, head_cols(1 - core, h)], place, xsend.at[i], xrecv.at[i], dev_core))
    local.append(pltpu.make_async_copy(
        q_hbm.at[:, half_cols(core)], qbuf.at[mine, :], local_sem.at[2 * heads]))
    swaps.append(remote(
        q_hbm.at[:, half_cols(1 - core)], qbuf.at[mine, :],
        xsend.at[2 * heads], xrecv.at[2 * heads], dev_core))

    for c in local:
        c.start()
    barrier = pltpu.get_barrier_semaphore()
    for dev in (dev_core, dev_x, dev_y):
        pl.semaphore_signal(
            barrier, inc=1, device_id={"seq": dev}, device_id_type=pl.DeviceIdType.MESH
        )

    @pl.when(has_up)
    def _():
        pl.semaphore_signal(
            barrier, inc=1, device_id={"seq": me + 8}, device_id_type=pl.DeviceIdType.MESH
        )

    @pl.when(has_down)
    def _():
        pl.semaphore_signal(
            barrier, inc=1, device_id={"seq": me - 8}, device_id_type=pl.DeviceIdType.MESH
        )

    steps = max(size // 8 - 1, 1)
    neighbours_up = 1 - plane // steps if size > 8 else 0
    neighbours_down = (plane + steps - 1) // steps if size > 8 else 0
    pl.semaphore_wait(barrier, 3 + neighbours_up + jnp.minimum(neighbours_down, 1))

    for c in swaps:
        c.start()

    def own_ready(h):
        for i in (2 * h, 2 * h + 1):
            local[i].wait()
            swaps[i].wait_recv()

    own_ready(0)
    start(ZB, 0)
    for h in range(1, heads):
        own_ready(h)
    for h in range(heads):
        cols = slice(h * HDIM, (h + 1) * HDIM)
        kf = feature(kbuf[h, j]).astype(jnp.bfloat16)
        dsum[0:HDIM, cols] = lax.dot_general(
            kf, vbuf[h, j], (((0,), (0,)), ((), ())), preferred_element_type=jnp.float32
        )
        norm = jnp.sum(kf.astype(jnp.float32), axis=0, keepdims=True)
        dsum[HDIM:, cols] = jnp.broadcast_to(norm, (PAD, HDIM))
    delta_send(0, dsum[...])
    start(AY, 0, ybit == 0)
    start(AX, 0, xbit == 0)
    local[2 * heads].wait()
    swaps[2 * heads].wait_recv()
    for h in range(min(2, heads)):
        fetch(h)
    pown[...] = jnp.zeros(pown.shape, jnp.float32)
    def first_forward():
        for kv in KV:
            arrive(ZB, 0, (kv,))
            start(ZC, 0, None, (kv,))
            start(BX, 0, None, (kv,))
            start(BY, 0, None, (kv,))
        if heads > 1:
            start(ZB, 1)
        dsum[...] += delta_arrive(0)
        delta_send(1, dsum[...])

    def first_old():
        for kv in KV:
            arrive(ZC, 0, (kv,))
            start(AY, 0, ybit == 1, (kv,))
            start(AX, 0, xbit == 1, (kv,))

    def first_plane():
        other = delta_arrive(1)
        dpre[...] = other * ybit.astype(jnp.float32)
        dsum[...] += other

        @pl.when(has_up & (plane == 0))
        def _():
            delta_send(2, dsum[...])

    def chain():
        @pl.when(has_down)
        def _():
            before = delta_arrive(2)
            dpre[...] += before

            @pl.when(has_up)
            def _():
                delta_send(2, before + dsum[...])

    def xor(a_bit, b_bit):
        return a_bit + b_bit - 2 * a_bit * b_bit

    def one_of(s, *steps):
        found = s == steps[0]
        for k in steps[1:]:
            found = found | (s == k)
        return found

    last_chain = 12

    def one_head(h, carry):
        attend(h, (j,), "own")

        @pl.when(h == 0)
        def _():
            first_forward()

        def look_ahead():
            @pl.when(h + 1 < heads)
            def _():
                relay(ZB, ZC, h + 1)

            @pl.when(h + 2 < heads)
            def _():
                start(ZB, h + 2)

        def step(s, c):
            old = one_of(s, 2, 3, 5)

            def slot_of(k):
                flip_x = jnp.where(one_of(k, 1, 3, 5, 6), 1, 0)
                flip_y = jnp.where(one_of(k, 2, 4, 5, 6), 1, 0)
                return jnp.where(one_of(k, 2, 3, 5), 0, 4) + xor(xbit, flip_x) + 2 * xor(ybit, flip_y)

            @pl.when(s == 1)
            def _():
                @pl.when(h == 0)
                def _():
                    first_old()

                look_ahead()

                @pl.when(two_down)
                def _():
                    attend(h, (8,), "old")

                relay(BX, BYF, h)

            @pl.when(s == 2)
            def _():
                relay(AY, AXF, h)

                @pl.when(h == 0)
                def _():
                    first_plane()

            @pl.when(s == 3)
            def _():
                when_head(h + 1, open_head)

                @pl.when(h == 2)
                def _():
                    project(0)

                arrive(AX, h)

            @pl.when(s == 4)
            def _():
                arrive(BY, h)

            @pl.when(s == 5)
            def _():
                arrive(AXF, h)

            @pl.when(s == 6)
            def _():
                arrive(BYF, h)

            @pl.when(7 * h + s == jnp.minimum(4 * plane, last_chain))
            def _():
                chain()

            @pl.when((h > 0) & (s == jnp.where(h == 1, 6, 2)))
            def _():
                finish(h - 1)

            @pl.when((h > 1) & (s == 6))
            def _():
                project(h - 1)

            bit = jnp.where(s == 3, xbit, ybit)
            held = jnp.where(old, jnp.where(bit == 1, 1, 0), jnp.where(has_down, 1, 0))
            alone = jnp.where(two_down, jnp.where(s == 0, 1, 0), held)

            @pl.when(alone == 1)
            def _():
                attend(h, (slot_of(s),))

            @pl.when(two_down & one_of(s, 2, 4, 6))
            def _():
                attend(h, (slot_of(s - 1), slot_of(s)))

            return c

        lax.fori_loop(0, 7, step, 0)
        return carry

    lax.fori_loop(0, heads, one_head, 0)
    if heads == 2:
        project(0)
    finish(heads - 1)
    project_last(heads - 1)

    def sent(h, carry):
        mix_copy(h).wait_send()
        return carry

    lax.fori_loop(0, heads, sent, 0)
    for c in swaps:
        c.wait_send()
    for i in (0, 1):
        delta_copy(i).wait_send()

    @pl.when(has_up)
    def _():
        delta_copy(2).wait_send()

    def all_sent(h, carry):
        for kind in plan:
            @pl.when(plan[kind][3])
            def _(kind=kind):
                for kv in KV:
                    copy_of(kind, h, kv).wait_send()
        return carry

    lax.fori_loop(0, heads, all_sent, 0)


def per_device(size, queries, keys, values, gate_logit, out_weight):
    rows = queries.shape[0]
    heads = gate_logit.shape[0]
    groups = keys.shape[1] // HDIM
    group_size = heads // groups
    assert WINDOW == 16 * rows and SEG == 4 * rows and size % 8 == 0 and groups % 2 == 0 and groups >= 4
    mine = groups // 2
    columns = out_weight.shape[1]
    qwidth = mine * group_size * HDIM
    f32, bf16 = jnp.float32, jnp.bfloat16
    vmem, anywhere = pl.BlockSpec(memory_space=pltpu.VMEM), pl.BlockSpec(memory_space=pl.ANY)
    dma = pltpu.SemaphoreType.DMA
    partial_value = pl.pallas_call(
        functools.partial(kernel, size, group_size),
        out_shape=jax.ShapeDtypeStruct((rows, columns), bf16),
        in_specs=[pl.BlockSpec(memory_space=pltpu.SMEM)] + [anywhere] * 4,
        out_specs=vmem,
        scratch_shapes=[
            pltpu.VMEM((2 * rows, qwidth), bf16),
            pltpu.VMEM((mine, 9, 2 * rows, HDIM), bf16),
            pltpu.VMEM((mine, 9, 2 * rows, HDIM), bf16),
            pltpu.VMEM((2 * rows * group_size, HDIM), f32),
            pltpu.VMEM((2, 2 * rows * group_size, 2 * HDIM), f32),
            pltpu.VMEM((mine, 2, rows, group_size * HDIM), bf16),
            pltpu.VMEM((mine, rows, group_size * HDIM), bf16),
            pltpu.VMEM((2, 2, group_size * HDIM, columns), bf16),
            pltpu.VMEM((rows, columns), f32),
            pltpu.VMEM((3, HDIM + PAD, mine * HDIM), bf16),
            pltpu.VMEM((3, HDIM + PAD, mine * HDIM), bf16),
            pltpu.VMEM((HDIM + PAD, mine * HDIM), f32),
            pltpu.VMEM((HDIM + PAD, mine * HDIM), f32),
            dma((2 * mine + 1,)),
            dma((2 * mine + 1,)),
            dma((2 * mine + 1,)),
            dma((8, mine, 2)),
            dma((8, mine, 2)),
            dma((3,)),
            dma((3,)),
            dma((mine,)),
            dma((mine,)),
            dma((mine, 2)),
        ],
        compiler_params=pltpu.CompilerParams(
            collective_id=0, has_side_effects=True, vmem_limit_bytes=60 * 1024 * 1024
        ),
    )(gate_logit, queries, keys, values, out_weight)
    return lax.psum_scatter(partial_value, "head", scatter_dimension=1, tiled=True)


def solution(mesh):
    in_specs = (P("seq", "head"), P("seq", "head"), P("seq", "head"), P("head"), P("head", None))
    out_specs = P("seq", "head")
    return jax.shard_map(
        functools.partial(per_device, mesh.shape["seq"]),
        mesh=mesh, in_specs=in_specs, out_specs=out_specs, check_vma=False,
    )
```

```python
import functools
import math

import jax
import jax.numpy as jnp
from jax import lax
from jax.experimental import pallas as pl
from jax.experimental.pallas import tpu as pltpu
from jax.sharding import PartitionSpec as P

HDIM = 128
WINDOW = 4096
SEG = 1024
LOG2E = 1.4426950408889634
EXP_SCALE = LOG2E / math.sqrt(HDIM)
TILE = 2048
PAD = 16
ZB, ZC, BX, BY, BYF, AX, AY, AXF = range(8)
KV = (0, 1)


def feature(source):
    wide = source.astype(jnp.float32)
    low = jnp.exp(jnp.minimum(wide, 0.0))
    return jnp.where(wide > 0.0, wide + 1.0, low)


def kernel(
    size, group_size, gate_ref, q_hbm, k_hbm, v_hbm, w_hbm, out_ref,
    qbuf, kbuf, vbuf, m_ref, acc_ref, mix, msend, wbuf, pown,
    wsend, wrecv, dsum, dpre,
    local_sem, xsend, xrecv, send_sem, recv_sem, dsend, drecv, psem, prsem, wsem,
):
    rows = q_hbm.shape[0]
    heads = kbuf.shape[0]
    width = heads * HDIM
    gwidth = group_size * HDIM
    qwidth = width * group_size
    own_q = heads * group_size
    blocks = 2 * group_size
    tiles = w_hbm.shape[1] // TILE
    me = lax.axis_index("seq")
    plane = me // 8
    p = me % 8
    core = p % 2
    xbit = (p // 2) % 2
    ybit = p // 4
    j = p // 2
    j_x = j + 1 - 2 * xbit
    j_y = j + 2 - 4 * ybit
    dev_core = me + 1 - 2 * core
    dev_x = me + 2 - 4 * xbit
    dev_y = me + 4 - 8 * ybit
    bufs = (kbuf, vbuf)
    has_up = me + 8 < size
    has_down = plane >= 1
    two_down = plane >= 2

    def remote(src, dst, ssem, rsem, dev):
        return pltpu.make_async_remote_copy(
            src_ref=src, dst_ref=dst, send_sem=ssem, recv_sem=rsem,
            device_id={"seq": dev}, device_id_type=pl.DeviceIdType.MESH,
        )

    plan = {
        ZB: (j, 4 + j, me + 8, has_up, has_down),
        ZC: (4 + j, 8, me + 8, has_up & has_down, two_down),
        BX: (4 + j, 4 + j, dev_x, has_down, has_down),
        BY: (4 + j, 4 + j, dev_y, has_down, has_down),
        BYF: (4 + j_x, 4 + j_x, dev_y, has_down, has_down),
        AX: (j + xbit * (8 - j), j, dev_x, (xbit == 0) | two_down, (xbit == 1) | two_down),
        AY: (j + ybit * (8 - j), j, dev_y, (ybit == 0) | two_down, (ybit == 1) | two_down),
        AXF: (j_y, j_y, dev_x, (ybit == 1) | two_down, (ybit == 1) | two_down),
    }

    def copy_of(kind, h, kv):
        src, dst, dev, _, _ = plan[kind]
        return remote(
            bufs[kv].at[h, src], bufs[kv].at[h, dst],
            send_sem.at[kind, h, kv], recv_sem.at[kind, h, kv], dev,
        )

    def start(kind, h, also=None, kvs=KV):
        ok = plan[kind][3] if also is None else plan[kind][3] & also

        @pl.when(ok)
        def _():
            for kv in kvs:
                copy_of(kind, h, kv).start()

    def arrive(kind, h, kvs=KV):
        @pl.when(plan[kind][4])
        def _():
            for kv in kvs:
                copy_of(kind, h, kv).wait_recv()

    def relay(kind, onward, h):
        for kv in KV:
            arrive(kind, h, (kv,))
            start(onward, h, None, (kv,))

    def open_head(h):
        arrive(ZC, h)
        for kind in (BX, AY, AX, BY):
            start(kind, h)

    def when_head(h, event):
        @pl.when(h < heads)
        def _():
            event(h)

    def delta_copy(i):
        dev = (dev_x, dev_y, me + 8)[i]
        return remote(wsend.at[i], wrecv.at[i], dsend.at[i], drecv.at[i], dev)

    def delta_send(i, value):
        wsend[i] = value.astype(jnp.bfloat16)
        delta_copy(i).start()

    def delta_arrive(i):
        delta_copy(i).wait_recv()
        return wrecv[i].astype(jnp.float32)

    def attend(h, slots, mask=None):
        qk_dims = (((1,), (1,)), ((), ()))

        def span(half):
            if mask == "own" and half == 0:
                return 0, rows
            if mask == "old" and half == 1:
                return rows, rows
            return 0, 2 * rows

        def block(i):
            return slice(i * rows, (i + 1) * rows)

        def scores(i):
            first, count = span(i % 2)
            cols = pl.ds(pl.multiple_of((h * group_size + i // 2) * HDIM, HDIM), HDIM)
            q = qbuf[(i % 2) * rows:(i % 2 + 1) * rows, cols]
            parts = [
                lax.dot_general(
                    q, kbuf[h, slot, first:first + count, :], qk_dims,
                    preferred_element_type=jnp.float32,
                )
                for slot in slots
            ]
            if mask is None:
                return jnp.concatenate(parts, axis=1) if len(parts) > 1 else parts[0]
            s, = parts
            qpos = lax.broadcasted_iota(jnp.int32, (rows, rows), 0)
            kpos = lax.broadcasted_iota(jnp.int32, (rows, rows), 1)
            allowed = (qpos >= kpos) if mask == "own" else (kpos > qpos)
            low = jnp.float32(-1e30)
            if count == rows:
                return jnp.where(allowed, s, low)
            if mask == "own":
                return jnp.concatenate([s[:, :rows], jnp.where(allowed, s[:, rows:], low)], axis=1)
            return jnp.concatenate([jnp.where(allowed, s[:, :rows], low), s[:, rows:]], axis=1)

        def soften(i, s):
            top = jnp.max(s, axis=1, keepdims=True)
            shape = (rows, HDIM)
            if mask == "own":
                new, alpha = jnp.broadcast_to(top, shape), None
            else:
                old = m_ref[block(i), :]
                new = jnp.maximum(old, top)
                alpha = jnp.exp2((old - new) * EXP_SCALE)
            m_ref[block(i), :] = new
            shift = jnp.concatenate([new] * (s.shape[1] // HDIM), axis=1)
            return jnp.exp2((s - shift) * EXP_SCALE).astype(jnp.bfloat16), alpha

        def gather(i, w, alpha):
            first, count = span(i % 2)
            pv = None
            for k, slot in enumerate(slots):
                v = vbuf[h, slot, first:first + count, :]
                wide = jnp.concatenate([v, jnp.ones((count, HDIM), jnp.bfloat16)], axis=1)
                one = jnp.dot(
                    w[:, k * count:(k + 1) * count], wide, preferred_element_type=jnp.float32
                )
                pv = one if pv is None else pv + one
            if alpha is None:
                acc_ref[h % 2, block(i), :] = pv
            else:
                acc_ref[h % 2, block(i), :] = (
                    acc_ref[h % 2, block(i), :] * jnp.concatenate([alpha, alpha], axis=1) + pv
                )

        waiting, ready = {}, {}
        for t in range(blocks + 2):
            if t < blocks:
                waiting[t] = scores(t)
            if 0 <= t - 1 < blocks:
                ready[t - 1] = soften(t - 1, waiting.pop(t - 1))
            if 0 <= t - 2 < blocks:
                gather(t - 2, *ready.pop(t - 2))

    def finish(h):
        cols = pl.ds(pl.multiple_of(h * HDIM, HDIM), HDIM)
        mem = dpre[0:HDIM, cols]
        high = mem.astype(jnp.bfloat16)
        low = (mem - high.astype(jnp.float32)).astype(jnp.bfloat16)
        norm = dpre[HDIM:HDIM + 1, cols]

        def part(place, target):
            def one(r, carry):
                n = h * group_size + r
                qcols = pl.ds(pl.multiple_of(n * HDIM, HDIM), HDIM)
                arows = pl.ds(pl.multiple_of((2 * r + place) * rows, rows), rows)
                qrows = pl.ds(pl.multiple_of(place * rows, rows), rows)
                qf = feature(qbuf[qrows, qcols]).astype(jnp.bfloat16)
                recalled = jnp.dot(qf, high, preferred_element_type=jnp.float32) + jnp.dot(
                    qf, low, preferred_element_type=jnp.float32
                )
                denominator = 1.0 + jnp.sum(qf.astype(jnp.float32) * norm, axis=1, keepdims=True)
                local_out = acc_ref[h % 2, arows, 0:HDIM] / acc_ref[h % 2, arows, HDIM:]
                share = jax.nn.sigmoid(jnp.full((1, HDIM), gate_ref[core * own_q + n], jnp.float32))
                mixed = share * (recalled / denominator) + (1.0 - share) * local_out
                target[:, pl.ds(pl.multiple_of(r * HDIM, HDIM), HDIM)] = mixed.astype(jnp.bfloat16)
                return carry

            lax.fori_loop(0, group_size, one, 0, unroll=True)

        part(1 - core, msend.at[h])
        mix_copy(h).start()
        part(core, mix.at[h, 0])

    def mix_copy(h):
        return remote(msend.at[h], mix.at[h, 1], psem.at[h], prsem.at[h], dev_core)

    def product(h, side, cols):
        return jnp.dot(mix[h, side], wbuf[h % 2, side, :, cols], preferred_element_type=jnp.float32)

    def weights(h):
        for side in (0, 1):
            owner = core + side * (1 - 2 * core)
            wrows = pl.ds(pl.multiple_of((owner * heads + h) * gwidth, gwidth), gwidth)
            yield pltpu.make_async_copy(w_hbm.at[wrows, :], wbuf.at[h % 2, side], wsem.at[h, side])

    def fetch(h):
        for c in weights(h):
            c.start()

    def fetched(h):
        for c in weights(h):
            c.wait()

    def tile_cols(i):
        return pl.ds(pl.multiple_of(i * TILE, TILE), TILE)

    def project(h):
        mix_copy(h).wait_recv()
        fetched(h)

        def one(i, carry):
            cols = tile_cols(i)
            pown[:, cols] += product(h, 0, cols) + product(h, 1, cols)
            return carry

        lax.fori_loop(0, tiles, one, 0)
        when_head(h + 2, fetch)

    def project_last(h):
        fetched(h)

        def one(i, carry):
            cols = tile_cols(i)
            pown[:, cols] += product(h, 0, cols)
            return carry

        lax.fori_loop(0, tiles, one, 0)
        mix_copy(h).wait_recv()

        def two(i, carry):
            cols = tile_cols(i)
            out_ref[:, cols] = (pown[:, cols] + product(h, 1, cols)).astype(jnp.bfloat16)
            return carry

        lax.fori_loop(0, tiles, two, 0)

    mine = pl.ds(pl.multiple_of(core * rows, rows), rows)
    hbms = (k_hbm, v_hbm)

    def head_cols(owner, h):
        return pl.ds(pl.multiple_of((owner * heads + h) * HDIM, HDIM), HDIM)

    def half_cols(owner):
        return pl.ds(pl.multiple_of(owner * qwidth, qwidth), qwidth)

    local, swaps = [], []
    for h in range(heads):
        for kv in KV:
            i = 2 * h + kv
            place = bufs[kv].at[h, j, mine, :]
            local.append(pltpu.make_async_copy(
                hbms[kv].at[:, head_cols(core, h)], place, local_sem.at[i]))
            swaps.append(remote(
                hbms[kv].at[:, head_cols(1 - core, h)], place, xsend.at[i], xrecv.at[i], dev_core))
    local.append(pltpu.make_async_copy(
        q_hbm.at[:, half_cols(core)], qbuf.at[mine, :], local_sem.at[2 * heads]))
    swaps.append(remote(
        q_hbm.at[:, half_cols(1 - core)], qbuf.at[mine, :],
        xsend.at[2 * heads], xrecv.at[2 * heads], dev_core))

    for c in local:
        c.start()
    barrier = pltpu.get_barrier_semaphore()
    for dev in (dev_core, dev_x, dev_y):
        pl.semaphore_signal(
            barrier, inc=1, device_id={"seq": dev}, device_id_type=pl.DeviceIdType.MESH
        )

    @pl.when(has_up)
    def _():
        pl.semaphore_signal(
            barrier, inc=1, device_id={"seq": me + 8}, device_id_type=pl.DeviceIdType.MESH
        )

    @pl.when(has_down)
    def _():
        pl.semaphore_signal(
            barrier, inc=1, device_id={"seq": me - 8}, device_id_type=pl.DeviceIdType.MESH
        )

    steps = max(size // 8 - 1, 1)
    neighbours_up = 1 - plane // steps if size > 8 else 0
    neighbours_down = (plane + steps - 1) // steps if size > 8 else 0
    pl.semaphore_wait(barrier, 3 + neighbours_up + jnp.minimum(neighbours_down, 1))

    for c in swaps:
        c.start()

    def own_ready(h):
        for i in (2 * h, 2 * h + 1):
            local[i].wait()
            swaps[i].wait_recv()

    own_ready(0)
    start(ZB, 0)
    for h in range(1, heads):
        own_ready(h)
    for h in range(heads):
        cols = slice(h * HDIM, (h + 1) * HDIM)
        kf = feature(kbuf[h, j]).astype(jnp.bfloat16)
        dsum[0:HDIM, cols] = lax.dot_general(
            kf, vbuf[h, j], (((0,), (0,)), ((), ())), preferred_element_type=jnp.float32
        )
        norm = jnp.sum(kf.astype(jnp.float32), axis=0, keepdims=True)
        dsum[HDIM:, cols] = jnp.broadcast_to(norm, (PAD, HDIM))
    delta_send(0, dsum[...])
    start(AY, 0, ybit == 0)
    start(AX, 0, xbit == 0)
    local[2 * heads].wait()
    swaps[2 * heads].wait_recv()
    for h in range(min(2, heads)):
        fetch(h)
    pown[...] = jnp.zeros(pown.shape, jnp.float32)
    def first_forward():
        for kv in KV:
            arrive(ZB, 0, (kv,))
            start(ZC, 0, None, (kv,))
            start(BX, 0, None, (kv,))
            start(BY, 0, None, (kv,))
        if heads > 1:
            start(ZB, 1)
        dsum[...] += delta_arrive(0)
        delta_send(1, dsum[...])

    def first_old():
        for kv in KV:
            arrive(ZC, 0, (kv,))
            start(AY, 0, ybit == 1, (kv,))
            start(AX, 0, xbit == 1, (kv,))

    def first_plane():
        other = delta_arrive(1)
        dpre[...] = other * ybit.astype(jnp.float32)
        dsum[...] += other

        @pl.when(has_up & (plane == 0))
        def _():
            delta_send(2, dsum[...])

    def chain():
        @pl.when(has_down)
        def _():
            before = delta_arrive(2)
            dpre[...] += before

            @pl.when(has_up)
            def _():
                delta_send(2, before + dsum[...])

    def xor(a_bit, b_bit):
        return a_bit + b_bit - 2 * a_bit * b_bit

    def one_of(s, *steps):
        found = s == steps[0]
        for k in steps[1:]:
            found = found | (s == k)
        return found

    last_chain = 12

    def one_head(h, carry):
        attend(h, (j,), "own")

        @pl.when(h == 0)
        def _():
            first_forward()

        def look_ahead(k):
            @pl.when(k < heads)
            def _():
                relay(ZB, ZC, k)

            @pl.when(k + 1 < heads)
            def _():
                start(ZB, k + 1)

        def step(s, c):
            old = one_of(s, 2, 3, 5)

            def slot_of(k):
                flip_x = jnp.where(one_of(k, 1, 3, 5, 6), 1, 0)
                flip_y = jnp.where(one_of(k, 2, 4, 5, 6), 1, 0)
                return jnp.where(one_of(k, 2, 3, 5), 0, 4) + xor(xbit, flip_x) + 2 * xor(ybit, flip_y)

            @pl.when(s == 1)
            def _():
                @pl.when(h == 0)
                def _():
                    first_old()
                    look_ahead(1)

                @pl.when(two_down)
                def _():
                    attend(h, (8,), "old")

                relay(BX, BYF, h)

            @pl.when(s == 2)
            def _():
                relay(AY, AXF, h)

                @pl.when(h == 0)
                def _():
                    first_plane()

            @pl.when(s == 3)
            def _():
                when_head(h + 1, open_head)

                @pl.when(h == 2)
                def _():
                    project(0)

                arrive(AX, h)

            @pl.when(s == 4)
            def _():
                arrive(BY, h)

            @pl.when(s == 5)
            def _():
                look_ahead(h + 2)
                arrive(AXF, h)

            @pl.when(s == 6)
            def _():
                arrive(BYF, h)

            @pl.when(7 * h + s == jnp.minimum(4 * plane, last_chain))
            def _():
                chain()

            @pl.when((h > 0) & (s == jnp.where(h == 1, 6, 2)))
            def _():
                finish(h - 1)

            @pl.when((h > 1) & (s == 6))
            def _():
                project(h - 1)

            bit = jnp.where(s == 3, xbit, ybit)
            held = jnp.where(old, jnp.where(bit == 1, 1, 0), jnp.where(has_down, 1, 0))
            alone = jnp.where(two_down, jnp.where(s == 0, 1, 0), held)

            @pl.when(alone == 1)
            def _():
                attend(h, (slot_of(s),))

            @pl.when(two_down & one_of(s, 2, 4, 6))
            def _():
                attend(h, (slot_of(s - 1), slot_of(s)))

            return c

        lax.fori_loop(0, 7, step, 0)
        return carry

    lax.fori_loop(0, heads, one_head, 0)
    if heads == 2:
        project(0)
    finish(heads - 1)
    project_last(heads - 1)

    def sent(h, carry):
        mix_copy(h).wait_send()
        return carry

    lax.fori_loop(0, heads, sent, 0)
    for c in swaps:
        c.wait_send()
    for i in (0, 1):
        delta_copy(i).wait_send()

    @pl.when(has_up)
    def _():
        delta_copy(2).wait_send()

    def all_sent(h, carry):
        for kind in plan:
            @pl.when(plan[kind][3])
            def _(kind=kind):
                for kv in KV:
                    copy_of(kind, h, kv).wait_send()
        return carry

    lax.fori_loop(0, heads, all_sent, 0)


def per_device(size, queries, keys, values, gate_logit, out_weight):
    rows = queries.shape[0]
    heads = gate_logit.shape[0]
    groups = keys.shape[1] // HDIM
    group_size = heads // groups
    assert WINDOW == 16 * rows and SEG == 4 * rows and size % 8 == 0 and groups % 2 == 0 and groups >= 4
    mine = groups // 2
    columns = out_weight.shape[1]
    qwidth = mine * group_size * HDIM
    f32, bf16 = jnp.float32, jnp.bfloat16
    vmem, anywhere = pl.BlockSpec(memory_space=pltpu.VMEM), pl.BlockSpec(memory_space=pl.ANY)
    dma = pltpu.SemaphoreType.DMA
    partial_value = pl.pallas_call(
        functools.partial(kernel, size, group_size),
        out_shape=jax.ShapeDtypeStruct((rows, columns), bf16),
        in_specs=[pl.BlockSpec(memory_space=pltpu.SMEM)] + [anywhere] * 4,
        out_specs=vmem,
        scratch_shapes=[
            pltpu.VMEM((2 * rows, qwidth), bf16),
            pltpu.VMEM((mine, 9, 2 * rows, HDIM), bf16),
            pltpu.VMEM((mine, 9, 2 * rows, HDIM), bf16),
            pltpu.VMEM((2 * rows * group_size, HDIM), f32),
            pltpu.VMEM((2, 2 * rows * group_size, 2 * HDIM), f32),
            pltpu.VMEM((mine, 2, rows, group_size * HDIM), bf16),
            pltpu.VMEM((mine, rows, group_size * HDIM), bf16),
            pltpu.VMEM((2, 2, group_size * HDIM, columns), bf16),
            pltpu.VMEM((rows, columns), f32),
            pltpu.VMEM((3, HDIM + PAD, mine * HDIM), bf16),
            pltpu.VMEM((3, HDIM + PAD, mine * HDIM), bf16),
            pltpu.VMEM((HDIM + PAD, mine * HDIM), f32),
            pltpu.VMEM((HDIM + PAD, mine * HDIM), f32),
            dma((2 * mine + 1,)),
            dma((2 * mine + 1,)),
            dma((2 * mine + 1,)),
            dma((8, mine, 2)),
            dma((8, mine, 2)),
            dma((3,)),
            dma((3,)),
            dma((mine,)),
            dma((mine,)),
            dma((mine, 2)),
        ],
        compiler_params=pltpu.CompilerParams(
            collective_id=0, has_side_effects=True, vmem_limit_bytes=60 * 1024 * 1024
        ),
    )(gate_logit, queries, keys, values, out_weight)
    return lax.psum_scatter(partial_value, "head", scatter_dimension=1, tiled=True)


def solution(mesh):
    in_specs = (P("seq", "head"), P("seq", "head"), P("seq", "head"), P("head"), P("head", None))
    out_specs = P("seq", "head")
    return jax.shard_map(
        functools.partial(per_device, mesh.shape["seq"]),
        mesh=mesh, in_specs=in_specs, out_specs=out_specs, check_vma=False,
    )
```
